32 devices in a mesh: dp: 8 (over y, x, core), mod: 4 (over z).
Axes of the slice: x: 2, y: 2, z: 4, core: 2. Of those that a mesh axis runs over, the one named last changes fastest.
Arguments:
- tokens: bfloat16 [2, 8, 1024, 2048], P(None, 'dp', 'mod'), may hold values from -6 to 6
- w_qkv: bfloat16 [3, 2048, 2048], P(None, 'dp', 'mod'), may hold values from -0.125 to 0.125
- w_out: bfloat16 [2048, 2048], P('mod', 'dp'), may hold values from -0.75 to 0.75
- w_up: bfloat16 [2048, 8192], P('dp', 'mod'), may hold values from -0.125 to 0.125
- w_down: bfloat16 [8192, 2048], P('mod', 'dp'), may hold values from -0.0625 to 0.0625
- gains: bfloat16 [2, 2048], P(None, 'dp'), may hold values from 0.5 to 1.5
- biases: bfloat16 [2, 2048], P(None, 'dp'), may hold values from -1.5 to 1.5
- cotangent: bfloat16 [2, 8, 1024, 2048], P(None, 'dp', 'mod'), may hold values from -6 to 6
- lengths: int32 [2, 8], P(None, 'dp'), may hold values from 256 to 1024, as said below
- positions: int32 [2, 8, 1024], P(None, 'dp'), may hold values from 0 to 1023, each once within a row
- flags: int32 [2, 8], P(None, 'dp'), may hold values 0 or 1
- item_weights: int32 [2, 8], P(None, 'dp'), may hold values from 1 to 8
Outputs:
- output: bfloat16 [2, 8, 1024, 2048], P(None, 'dp', 'mod')
- input_grad: float32 [2, 8, 1024, 2048], P(None, 'dp', 'mod')
- grad_w_qkv: float32 [3, 2048, 2048], P(None, 'dp', 'mod')
- grad_w_out: float32 [2048, 2048], P('mod', 'dp')
- grad_w_up: float32 [2048, 8192], P('dp', 'mod')
- grad_w_down: float32 [8192, 2048], P('mod', 'dp')
- grad_gains: float32 [2, 2048], P(None, 'dp')
- grad_biases: float32 [2, 2048], P(None, 'dp')
The draws below stay inside these ranges and needn't reach their ends.
Inputs may be any that keep to these rules, and one draw needn't show every extreme that they name: `lengths`: live positions of each item; in every micro-batch at least one item has all 1024. Each item's row is a permutation: slot s holds sequence place positions[m, i, s].
All inputs are finite; a program needn't handle non-finite values. No bound on the sum of `flags` on one device may be relied on, other than what follows from the above.
Results may differ from the reference program's by a relative error of at most 0.02.
Values may be sent and summed in bfloat16 or wider, within the bound.
A program may use at most 184 MiB of HBM per device.

```python
import math
import jax
import jax.numpy as jnp
from jax import lax

D = 2048
H = 16
HD = 128
FF = 8192
SLOT = 1024
QBLOCK = 512
MICRO = 2
ITEMS = 8


def draw_lengths(key, part):
    full_key, short_key, pick_key = jax.random.split(key, 3)
    full_item = jax.random.randint(full_key, (MICRO, ITEMS), 0, 4) == 0
    short_len = jax.random.randint(short_key, (MICRO, ITEMS), SLOT // 4, SLOT * 3 // 4 + 1)
    chosen = jax.random.randint(pick_key, (MICRO, 1), 0, ITEMS)
    forced = jnp.arange(ITEMS)[None, :] == chosen
    return jnp.where(full_item | forced, SLOT, short_len).astype(jnp.int32)


def with_ends(entries, key, least, largest):
    index_at = [jax.random.randint(jax.random.fold_in(key, axis), (), 0, length) for axis, length in enumerate(entries.shape)]
    widest = entries.shape.index(max(entries.shape))
    beside = index_at[:widest] + [(index_at[widest] + 1) % entries.shape[widest]] + index_at[widest + 1:]
    return entries.at[tuple(index_at)].set(least).at[tuple(beside)].set(largest)


def levels(key, extent, cuts, least, high):
    loudness, own = 1.0, jax.random.fold_in(key, 6)
    for position, shards_of in cuts:
        heights = jnp.exp(jax.random.uniform(jax.random.fold_in(own, position), (shards_of,), jnp.float32, least / len(cuts), high / len(cuts)))
        loudness = loudness * jnp.repeat(heights, extent[position] // shards_of).reshape([-1 if axis == position else 1 for axis in range(len(extent))])
    return loudness


def noise(rng, dims, deviation, most, cuts=(), kind=jnp.bfloat16):
    values = deviation * jax.random.normal(rng, dims, jnp.float32)
    if cuts:
        values = values * levels(rng, dims, cuts, -0.22, 0.18)
    return jnp.clip(values, -most, most).astype(kind)


def setup_inputs(seed: int = 0) -> dict:
    seeds = jax.random.split(jax.random.key(seed), 13)
    return {
        "tokens": noise(seeds[0], (MICRO, ITEMS, SLOT, D), 1.0, 6.0, ((1, 8), (2, 4))),
        "w_qkv": noise(seeds[1], (3, D, H * HD), D ** -0.5, 0.125, ((1, 8), (2, 4))),
        "w_out": noise(seeds[2], (H * HD, D), (H * HD // 32) ** -0.5, 0.75, ((0, 4), (1, 8))),
        "w_up": noise(seeds[3], (D, FF), D ** -0.5, 0.125, ((0, 8), (1, 4))),
        "w_down": noise(seeds[4], (FF, D), FF ** -0.5, 0.0625, ((0, 4), (1, 8))),
        "gains": jnp.clip(1.0 + 0.1 * jax.random.normal(seeds[5], (2, D), jnp.float32), 0.5, 1.5).astype(jnp.bfloat16),
        "biases": noise(seeds[6], (2, D), 0.3, 1.5, ((1, 8),)),
        "cotangent": noise(seeds[7], (MICRO, ITEMS, SLOT, D), 1.0, 6.0, ((1, 8), (2, 4))),
        "lengths": draw_lengths(jax.random.fold_in(seeds[12], 71), 0),
        "positions": jax.vmap(lambda own: jax.random.permutation(own, SLOT))(jax.random.split(seeds[9], MICRO * ITEMS)).reshape((MICRO, ITEMS, SLOT)).astype(jnp.int32),
        "flags": with_ends((jax.random.randint(seeds[10], (MICRO, ITEMS), 0, 4) < 1).astype(jnp.int32), jax.random.fold_in(seeds[10], 1), 0, 1),
        "item_weights": with_ends(jax.random.randint(seeds[11], (MICRO, ITEMS), 1, 9), jax.random.fold_in(seeds[11], 1), 1, 8).astype(jnp.int32),
    }


@jax.custom_vjp
def low(v):
    return lax.optimization_barrier(v.astype(jnp.bfloat16)).astype(jnp.float32)

@jax.custom_vjp
def low_back(v):
    return v

def low_keep(v):
    return (low(v), None)

def low_pass(kept, grad):
    return (grad,)

def back_keep(v):
    return (v, None)

def back_low(kept, grad):
    return (low(grad),)
low.defvjp(low_keep, low_pass)
low_back.defvjp(back_keep, back_low)
EPS = 1e-05
PRECISE = lax.Precision.HIGHEST
MASKED_SCORE = -1e+30

def layer_norm(features, norm_gain, norm_bias):
    row_mean = lax.optimization_barrier(jnp.mean(features, axis=-1, keepdims=True))
    centred = features - row_mean
    row_var = lax.optimization_barrier(jnp.mean(centred * centred, axis=-1, keepdims=True))
    return centred * lax.rsqrt(row_var + EPS) * norm_gain + norm_bias

def item_layer(params, tok_rows, places, length):
    w_qkv, w_out, w_up, w_down, gains, biases = params
    normed = low(layer_norm(tok_rows, gains[0], biases[0]))
    projected = low(low_back(jnp.einsum('sd,tdc->tsc', normed, w_qkv, precision=PRECISE)))
    heads_all = projected.reshape(3, SLOT, H, HD)
    queries = heads_all[0]
    key_heads = heads_all[1]
    value_heads = heads_all[2]
    scaling = 1.0 / math.sqrt(HD)

    def block_attend(start):
        query_block = lax.dynamic_slice_in_dim(queries, start, QBLOCK, 0)
        query_places = lax.dynamic_slice_in_dim(places, start, QBLOCK, 0)
        raw_score = low_back(jnp.einsum('qhe,khe->hqk', query_block, key_heads, precision=PRECISE))
        visible = (places[None, :] <= query_places[:, None]) & (places[None, :] < length)
        scores = jnp.where(visible[None], raw_score * scaling, MASKED_SCORE)
        row_max = lax.optimization_barrier(jnp.max(scores, axis=-1, keepdims=True))
        exponent = jnp.exp(scores - row_max)
        attn_prob = low(exponent / lax.optimization_barrier(jnp.sum(exponent, axis=-1, keepdims=True)))
        return jnp.einsum('hqk,khe->qhe', attn_prob, value_heads, precision=PRECISE)
    starts = (jnp.arange(SLOT // QBLOCK) * QBLOCK).astype(jnp.int32)
    mixed = lax.map(jax.checkpoint(block_attend), starts)
    mixed = low(low_back(mixed.reshape(SLOT, H * HD)))
    branch = low_back(jnp.dot(mixed, w_out, precision=PRECISE))
    hidden = tok_rows + branch
    normed_two = low(layer_norm(hidden, gains[1], biases[1]))
    upper_pre = low_back(jnp.dot(normed_two, w_up, precision=PRECISE))
    active = low(jax.nn.gelu(upper_pre, approximate=True))
    return hidden + low_back(jnp.dot(active, w_down, precision=PRECISE))

def reference(tokens, w_qkv, w_out, w_up, w_down, gains, biases, cotangent, lengths, positions, flags, item_weights):
    params = (w_qkv.astype(jnp.float32), w_out.astype(jnp.float32), w_up.astype(jnp.float32), w_down.astype(jnp.float32), gains.astype(jnp.float32), biases.astype(jnp.float32))
    item_total = MICRO * ITEMS
    tok_rows = tokens.astype(jnp.float32).reshape(item_total, SLOT, D)
    places = positions.reshape(item_total, SLOT).astype(jnp.int32)
    length_all = lengths.reshape(item_total).astype(jnp.int32)

    def forward(params_in, rows_in):

        def item_fn(packed):
            return item_layer(params_in, packed[0], packed[1], packed[2])
        return lax.map(jax.checkpoint(item_fn), (rows_in, places, length_all))
    outputs, pullback = jax.vjp(forward, params, tok_rows)
    item_scale = jnp.where(flags == 1, item_weights.astype(jnp.float32) / 4.0, 1.0).reshape(item_total)
    live_slots = (places < length_all[:, None]).astype(jnp.float32)
    scaled = cotangent.astype(jnp.float32).reshape(item_total, SLOT, D) * (item_scale[:, None] * live_slots)[:, :, None]
    param_grads, input_grad = pullback(scaled)
    full_shape = (MICRO, ITEMS, SLOT, D)
    return (outputs.astype(jnp.bfloat16).reshape(full_shape), input_grad.reshape(full_shape), param_grads[0], param_grads[1], param_grads[2], param_grads[3], param_grads[4], param_grads[5])
```

```python
import math

import jax
import jax.numpy as jnp
from jax import lax
from jax.sharding import PartitionSpec as P

HD = 128
QBLOCK = 512
EPS = 1e-05
MASKED_SCORE = -1e30
BF = jnp.bfloat16
F32 = jnp.float32
AXES = ("dp", "mod")


def gelu_tanh(upper_pre):
    return jax.nn.gelu(upper_pre, approximate=True)


def gelu_grad(upper_pre, grad_active):
    return jax.vjp(gelu_tanh, upper_pre)[1](grad_active)[0]


def norm_parts(rows):
    mean = jnp.mean(rows, axis=-1, keepdims=True)
    centred = rows - mean
    var = jnp.mean(centred * centred, axis=-1, keepdims=True)
    inv = lax.rsqrt(var + EPS)
    return centred * inv, inv


def norm_back(grad, gain, unit, inv):
    e = grad * gain
    mean_e = jnp.mean(e, axis=-1, keepdims=True)
    mean_ex = jnp.mean(e * unit, axis=-1, keepdims=True)
    return inv * (e - mean_e - unit * mean_ex)


def bit_list(n):
    return [1 << b for b in range(n.bit_length() - 1)]


def bit_reverse(i, n):
    out = 0
    for b in bit_list(n):
        out = out * 2 + (1 if i & b else 0)
    return out


class Plan:
    def __init__(self, n_dp, n_mod, micro):
        self.group = n_mod
        self.slabs = n_dp // n_mod
        self.n_mod = n_mod
        self.micro = micro
        self.span = n_mod // micro
        self.owner = [bit_reverse(z, n_mod) for z in range(n_mod)]

    def dev(self, y, q, z):
        return (y * self.group + q) * self.n_mod + z

    def all(self, f):
        return [
            (self.dev(y, q, z), self.dev(*f(y, q, z)))
            for y in range(self.slabs)
            for q in range(self.group)
            for z in range(self.n_mod)
        ]

    def swap_q(self, x, bit):
        return lax.ppermute(x, AXES, self.all(lambda y, q, z: (y, q ^ bit, z)))

    def swap_y(self, x, bit):
        return lax.ppermute(x, AXES, self.all(lambda y, q, z: (y ^ bit, q, z)))

    def move(self, k):
        def to(y, q, z):
            m = (k - q // self.span) % self.micro
            return y, self.owner[z], m * self.span + q % self.span

        return self.all(to)

    def send(self, x, k):
        return lax.ppermute(x, AXES, self.move(k))

    def send_back(self, x, k):
        return lax.ppermute(x, AXES, [(b, a) for a, b in self.move(k)])

    def gather(self, x):
        blocks = {0: x}
        for bit in reversed(bit_list(self.group)):
            for r in list(blocks):
                blocks[r | bit] = self.swap_q(blocks[r], bit)
        return jnp.concatenate([blocks[r] for r in range(self.group)], axis=0)

    def scatter(self, parts):
        rows = parts.shape[0] // self.group
        held = {r: parts[r * rows : (r + 1) * rows] for r in range(self.group)}
        for bit in bit_list(self.group):
            merged = {}
            for r in held:
                if not r & bit:
                    merged[r] = held[r].astype(F32) + self.swap_q(
                        held[r | bit].astype(BF), bit
                    ).astype(F32)
            held = merged
        return held[0]

    def exchange(self, x, q):
        for bit in bit_list(self.group):
            hi, lo = self.group // (2 * bit), bit
            view = x.reshape((hi, 2, lo) + x.shape[1:])
            mine = (q // bit) % 2
            keep = lax.dynamic_index_in_dim(view, mine, 1, keepdims=False)
            give = lax.dynamic_index_in_dim(view, 1 - mine, 1, keepdims=False)
            got = self.swap_q(give, bit)
            low = jnp.where(mine == 0, keep, got)
            high = jnp.where(mine == 0, got, keep)
            x = jnp.stack([low, high], axis=1).reshape(x.shape)
        return x


def shards(plan, n_dp, n_mod, args):
    (
        tokens,
        w_qkv,
        w_out,
        w_up,
        w_down,
        gains,
        biases,
        cotangent,
        lengths,
        positions,
        flags,
        item_weights,
    ) = args
    micro, _, rows_here, width = tokens.shape
    slots = positions.shape[2]
    group, slabs, span = plan.group, plan.slabs, plan.span
    block = width // n_dp
    half = width // slabs
    d = lax.axis_index("dp")
    z = lax.axis_index("mod")
    y = d // group
    q = d % group
    head_cols = w_qkv.shape[2]
    heads_here = head_cols // HD
    head_sub = head_cols // group
    ffn_cols = w_up.shape[1]
    ffn_sub = ffn_cols // group
    scaling = 1.0 / math.sqrt(HD)

    def turn(x):
        parts = x.reshape(x.shape[:-1] + (slabs, half))
        return jnp.concatenate(
            [
                lax.dynamic_index_in_dim(parts, y ^ r, x.ndim - 1, keepdims=False)
                for r in range(slabs)
            ],
            axis=-1,
        )

    small = jnp.concatenate(
        [
            positions.astype(F32).reshape(-1),
            gains.astype(F32).reshape(-1),
            biases.astype(F32).reshape(-1),
            lengths.astype(F32).reshape(-1),
            flags.astype(F32).reshape(-1),
            item_weights.astype(F32).reshape(-1),
        ]
    )
    every = lax.all_gather(small, "dp", axis=0)
    cut = micro * slots
    place_all = every[:, :cut].reshape(n_dp, micro, slots)
    gain_all = every[:, cut : cut + 2 * block].reshape(n_dp, 2, block)
    bias_all = every[:, cut + 2 * block : cut + 4 * block].reshape(n_dp, 2, block)
    facts = every[:, cut + 4 * block :].reshape(n_dp, 3, micro)
    gain_vals = turn(jnp.swapaxes(gain_all, 0, 1).reshape(2, width))
    bias_vals = turn(jnp.swapaxes(bias_all, 0, 1).reshape(2, width))
    my_micro = z // span
    order = jnp.array([plan.owner.index(i) for i in range(group)], jnp.int32)
    block_of = order[q ^ jnp.arange(group)]

    def spread_qkv():
        parts = jnp.moveaxis(w_qkv.reshape(3, block, group, head_sub), 2, 0)
        got = plan.exchange(parts, q)
        mine = jnp.moveaxis(got, 0, 1).reshape(3, half, head_sub)
        wide = lax.all_gather(mine, "mod", axis=2, tiled=True)
        return jnp.concatenate([wide, plan.swap_y(wide, 1)], axis=1)

    def spread_out():
        got = plan.exchange(w_out.reshape(group, head_sub, block), q)
        mine = jnp.swapaxes(got, 0, 1).reshape(head_sub, half)
        wide = lax.all_gather(mine, "mod", axis=0, tiled=True)
        return jnp.concatenate([wide, plan.swap_y(wide, 1)], axis=1)

    def spread_up():
        parts = jnp.swapaxes(w_up.reshape(block, group, ffn_sub), 0, 1)
        mine = plan.exchange(parts, q).reshape(half, ffn_sub)
        wide = lax.all_gather(mine, "mod", axis=1, tiled=True)
        return jnp.concatenate([wide, plan.swap_y(wide, 1)], axis=0)

    def spread_down():
        got = plan.exchange(w_down.reshape(group, ffn_sub, block), q)
        mine = jnp.swapaxes(got, 0, 1).reshape(ffn_sub, half)
        wide = lax.all_gather(mine, "mod", axis=0, tiled=True)
        return jnp.concatenate([wide, plan.swap_y(wide, 1)], axis=1)

    full_qkv = spread_qkv()
    full_out = spread_out()
    full_up = spread_up()
    full_down = spread_down()

    def block_for(x, k):
        m = (k - q // span) % micro
        return turn(lax.dynamic_index_in_dim(x, m, 0, keepdims=False)[0])

    def attend(query_block, keys, query_places, places, length):
        raw = jnp.einsum("qhe,khe->hqk", query_block, keys, preferred_element_type=F32)
        visible = (places[None, :] <= query_places[:, None]) & (places[None, :] < length)
        scores = jnp.where(visible[None], raw * scaling, MASKED_SCORE)
        top = jnp.max(scores, axis=-1, keepdims=True)
        exponent = jnp.exp(scores - top)
        return exponent / jnp.sum(exponent, axis=-1, keepdims=True)

    state = []
    for k in range(micro):
        rows = plan.send(block_for(tokens, k), k).astype(F32)
        pair = (k - my_micro) % micro
        source = y * group + pair * span + z % span
        item = lax.dynamic_index_in_dim(place_all, source, 0, keepdims=False)
        places = lax.dynamic_index_in_dim(item, my_micro, 0, keepdims=False)
        places = places.reshape(group, rows_here)[block_of].reshape(-1)
        fact = lax.dynamic_index_in_dim(facts, source, 0, keepdims=False)
        fact = lax.dynamic_index_in_dim(fact, my_micro, 1, keepdims=False)
        length = fact[0]
        scale = jnp.where(fact[1] == 1.0, fact[2] / 4.0, 1.0)
        unit_one, inv_one = norm_parts(rows)
        normed = (unit_one * gain_vals[0] + bias_vals[0]).astype(BF)
        normed_all = plan.gather(normed)
        projected = jnp.einsum(
            "sd,tdc->tsc", normed_all, full_qkv, preferred_element_type=F32
        ).astype(BF)
        split = projected.reshape(3, slots, heads_here, HD)
        mixed_parts = []
        for start in range(0, slots, QBLOCK):
            prob = attend(
                split[0, start : start + QBLOCK],
                split[1],
                places[start : start + QBLOCK],
                places,
                length,
            )
            mixed_parts.append(
                jnp.einsum("hqk,khe->qhe", prob.astype(BF), split[2], preferred_element_type=F32)
            )
        mixed = jnp.concatenate(mixed_parts, axis=0).reshape(slots, head_cols).astype(BF)
        branch = plan.scatter(
            jnp.einsum("sc,cd->sd", mixed, full_out, preferred_element_type=F32).astype(BF)
        )
        hidden = rows + branch
        unit_two, inv_two = norm_parts(hidden)
        normed_two = (unit_two * gain_vals[1] + bias_vals[1]).astype(BF)
        normed_two_all = plan.gather(normed_two)
        upper_pre = jnp.einsum("sd,df->sf", normed_two_all, full_up, preferred_element_type=F32)
        active = gelu_tanh(upper_pre).astype(BF)
        ffn = plan.scatter(
            jnp.einsum("sf,fd->sd", active, full_down, preferred_element_type=F32).astype(BF)
        )
        output = plan.send_back(turn((hidden + ffn).astype(BF)), k)

        factor = scale * (places[:rows_here] < length).astype(F32)
        grad_out = plan.send(block_for(cotangent, k), k).astype(F32) * factor[:, None]
        grad_out_all = plan.gather(grad_out.astype(BF))
        grad_active = jnp.einsum(
            "sd,fd->sf", grad_out_all, full_down, preferred_element_type=F32
        )
        grad_upper = gelu_grad(upper_pre, grad_active).astype(BF)
        grad_two = plan.scatter(
            jnp.einsum("sf,df->sd", grad_upper, full_up, preferred_element_type=F32).astype(BF)
        )
        grad_hidden = grad_out + norm_back(grad_two, gain_vals[1], unit_two, inv_two)
        grad_hidden_all = plan.gather(grad_hidden.astype(BF))
        grad_mixed = jnp.einsum(
            "sd,cd->sc", grad_hidden_all, full_out, preferred_element_type=F32
        ).astype(BF)
        grad_mixed = grad_mixed.reshape(slots, heads_here, HD)
        grad_keys = grad_values = 0.0
        query_parts = []
        for start in range(0, slots, QBLOCK):
            query_block = split[0, start : start + QBLOCK]
            prob = attend(
                query_block, split[1], places[start : start + QBLOCK], places, length
            )
            grad_block = grad_mixed[start : start + QBLOCK]
            grad_values = grad_values + jnp.einsum(
                "hqk,qhe->khe", prob.astype(BF), grad_block, preferred_element_type=F32
            )
            grad_prob = jnp.einsum(
                "qhe,khe->hqk", grad_block, split[2], preferred_element_type=F32
            )
            inner = jnp.sum(prob * grad_prob, axis=-1, keepdims=True)
            grad_raw = (prob * (grad_prob - inner) * scaling).astype(BF)
            query_parts.append(
                jnp.einsum("hqk,khe->qhe", grad_raw, split[1], preferred_element_type=F32)
            )
            grad_keys = grad_keys + jnp.einsum(
                "hqk,qhe->khe", grad_raw, query_block, preferred_element_type=F32
            )
        grad_proj = (
            jnp.stack([jnp.concatenate(query_parts, axis=0), grad_keys, grad_values])
            .astype(BF)
            .reshape(3, slots, head_cols)
        )
        grad_one = plan.scatter(
            jnp.einsum("tsc,tdc->sd", grad_proj, full_qkv, preferred_element_type=F32).astype(BF)
        )
        input_grad = grad_hidden + norm_back(grad_one, gain_vals[0], unit_one, inv_one)
        input_grad = plan.send_back(turn(input_grad.astype(BF)), k)
        sums = jnp.stack(
            [
                jnp.sum(grad_one * unit_one, axis=0),
                jnp.sum(grad_two * unit_two, axis=0),
                jnp.sum(grad_one, axis=0),
                jnp.sum(grad_two, axis=0),
            ]
        )
        state.append(
            dict(
                output=output,
                input_grad=input_grad,
                sums=sums,
                normed=normed_all,
                proj=grad_proj,
                mixed=mixed,
                grad_hidden=grad_hidden_all,
                normed_two=normed_two_all,
                grad_upper=grad_upper,
                active=active,
                grad_out=grad_out_all,
            )
        )

    def total(spec, left, right):
        out = 0.0
        for s in state:
            out = out + jnp.einsum(spec, s[left], s[right], preferred_element_type=F32)
        return out.astype(BF)

    def both(mine, other):
        return (mine.astype(F32) + plan.swap_y(other, 1).astype(F32)).astype(BF)

    def settle(part, axis):
        return lax.psum_scatter(part, "mod", scatter_dimension=axis, tiled=True)

    dw_down = total("sf,sd->fd", "active", "grad_out")
    dw_up = total("sd,sf->df", "normed_two", "grad_upper")
    dw_out = total("sc,sd->cd", "mixed", "grad_hidden")
    dw_qkv = total("sd,tsc->tdc", "normed", "proj")

    part = settle(both(dw_down[:, :half], dw_down[:, half:]), 0)
    part = plan.exchange(jnp.swapaxes(part.reshape(ffn_sub, group, block), 0, 1), q)
    grad_down = part.reshape(ffn_cols, block).astype(F32)

    part = settle(both(dw_up[:half], dw_up[half:]), 1)
    part = plan.exchange(part.reshape(group, block, ffn_sub), q)
    grad_up = jnp.swapaxes(part, 0, 1).reshape(block, ffn_cols).astype(F32)

    part = settle(both(dw_out[:, :half], dw_out[:, half:]), 0)
    part = plan.exchange(jnp.swapaxes(part.reshape(head_sub, group, block), 0, 1), q)
    grad_out_w = part.reshape(head_cols, block).astype(F32)

    part = settle(both(dw_qkv[:, :half], dw_qkv[:, half:]), 2)
    part = plan.exchange(jnp.moveaxis(part.reshape(3, group, block, head_sub), 1, 0), q)
    grad_qkv = jnp.moveaxis(part, 0, 2).reshape(3, block, head_cols).astype(F32)

    sums = lax.psum(turn(state[0]["sums"] + state[1]["sums"]), AXES)
    mine = lax.dynamic_slice_in_dim(sums, d * block, block, 1)

    def in_order(name):
        stacked = jnp.stack([s[name] for s in state])
        pick = (jnp.arange(micro) + q // span) % micro
        return stacked[pick][:, None]

    return (
        in_order("output"),
        in_order("input_grad").astype(F32),
        grad_qkv,
        grad_out_w,
        grad_up,
        grad_down,
        mine[:2],
        mine[2:],
    )


def solution(mesh):
    n_dp, n_mod = mesh.shape["dp"], mesh.shape["mod"]

    def body(*args):
        plan = Plan(n_dp, n_mod, args[0].shape[0])
        return shards(plan, n_dp, n_mod, args)

    in_specs = (
        P(None, "dp", "mod", None),
        P(None, "dp", "mod"),
        P("mod", "dp"),
        P("dp", "mod"),
        P("mod", "dp"),
        P(None, "dp"),
        P(None, "dp"),
        P(None, "dp", "mod", None),
        P(None, "dp"),
        P(None, "dp", None),
        P(None, "dp"),
        P(None, "dp"),
    )
    out_specs = (
        P(None, "dp", "mod", None),
        P(None, "dp", "mod", None),
        P(None, "dp", "mod"),
        P("mod", "dp"),
        P("dp", "mod"),
        P("mod", "dp"),
        P(None, "dp"),
        P(None, "dp"),
    )
    return jax.shard_map(body, mesh=mesh, in_specs=in_specs, out_specs=out_specs, check_vma=False)
```

```python
import functools
import math

import jax
import jax.numpy as jnp
from jax import lax
from jax.experimental import pallas as pl
from jax.experimental.pallas import tpu as pltpu
from jax.sharding import PartitionSpec as P

HD = 128
QBLOCK = 512
LOG_SCALE = math.log2(math.e) / math.sqrt(HD)
NOT_A_KEY = 1e9
EPS = 1e-05
MASKED_SCORE = -1e30
BF = jnp.bfloat16
F32 = jnp.float32
AXES = ("dp", "mod")


def gelu_and_slope(u):
    c = math.sqrt(2.0 / math.pi)
    square = u * u
    t = jnp.tanh(c * u * (1.0 + 0.044715 * square))
    half = 0.5 * (1.0 + t)
    slope = half + 0.5 * u * (1.0 - t * t) * (c * (1.0 + 3 * 0.044715 * square))
    return u * half, slope


def dot_nt(a, b):
    return lax.dot_general(a, b, (((1,), (1,)), ((), ())), preferred_element_type=F32)


def dot_nn(a, b):
    return lax.dot_general(a, b, (((1,), (0,)), ((), ())), preferred_element_type=F32)


def dot_tn(a, b):
    return lax.dot_general(a, b, (((0,), (0,)), ((), ())), preferred_element_type=F32)


def attend_kernel(step_rows, queries, keys, values, query_place, key_place, out, log_sum):
    keys, values, kp = keys[...], values[...], key_place[...]

    def step(i, _):
        at = pl.ds(pl.multiple_of(i * step_rows, step_rows), step_rows)
        raw = dot_nt(queries[at, :], keys)
        raw = jnp.where(kp <= query_place[at, :], raw, MASKED_SCORE)
        top = jnp.max(raw, axis=-1, keepdims=True)
        e = jnp.exp2((raw - top) * LOG_SCALE)
        total = jnp.sum(e, axis=-1, keepdims=True)
        out[at, :] = (dot_nn(e.astype(BF), values) / total).astype(BF)
        log_sum[0, at, :] = top * LOG_SCALE + jnp.log2(total)
        return 0

    lax.fori_loop(0, queries.shape[0] // step_rows, step, 0, unroll=2)


def attend_back_kernel(
    step_rows,
    queries,
    keys,
    values,
    mixed,
    grad,
    log_sum,
    query_place,
    key_place,
    out,
    grad_keys,
    grad_values,
):
    keys, values, kp = keys[...], values[...], key_place[...]
    scaling = 1.0 / math.sqrt(HD)
    grad_keys[...] = jnp.zeros_like(grad_keys)
    grad_values[...] = jnp.zeros_like(grad_values)

    def step(i, _):
        at = pl.ds(pl.multiple_of(i * step_rows, step_rows), step_rows)
        query, g = queries[at, :], grad[at, :]
        raw = dot_nt(query, keys)
        prob = jnp.where(
            kp <= query_place[at, :], jnp.exp2(raw * LOG_SCALE - log_sum[0, at, :]), 0.0
        )
        inner = jnp.sum(g.astype(F32) * mixed[at, :].astype(F32), axis=-1, keepdims=True)
        grad_raw = (prob * (dot_nt(g, values) - inner)).astype(BF)
        grad_values[...] += dot_tn(prob.astype(BF), g)
        grad_keys[...] += dot_tn(grad_raw, query)
        out[0, at, :] = (dot_nn(grad_raw, keys) * scaling).astype(BF)
        return 0

    lax.fori_loop(0, queries.shape[0] // step_rows, step, 0, unroll=2)
    out[1] = (grad_keys[...] * scaling).astype(BF)
    out[2] = grad_values[...].astype(BF)


def attend_specs(slots):
    return (
        pl.BlockSpec((3, slots, HD), lambda h: (0, 0, h)),
        pl.BlockSpec((slots, HD), lambda h: (0, h)),
        pl.BlockSpec((1, slots, 1), lambda h: (h, 0, 0)),
        pl.BlockSpec((slots, 1), lambda h: (0, 0)),
        pl.BlockSpec((1, slots), lambda h: (0, 0)),
    )


def attend(proj, query_place, key_place):
    slots, cols = proj[0].shape
    three, one, sums, column, row = attend_specs(slots)
    return pl.pallas_call(
        functools.partial(attend_kernel, QBLOCK),
        grid=(cols // HD,),
        in_specs=[one, one, one, column, row],
        out_specs=[one, sums],
        out_shape=[
            jax.ShapeDtypeStruct((slots, cols), BF),
            jax.ShapeDtypeStruct((cols // HD, slots, 1), F32),
        ],
        cost_estimate=pl.CostEstimate(
            flops=8 * slots * slots * cols,
            bytes_accessed=8 * slots * cols,
            transcendentals=cols // HD * slots * slots,
        ),
        compiler_params=pltpu.CompilerParams(vmem_limit_bytes=40 << 20),
    )(*proj, query_place, key_place)


def attend_back(proj, mixed, grad, log_sum, query_place, key_place):
    slots, cols = proj[0].shape
    three, one, sums, column, row = attend_specs(slots)
    return pl.pallas_call(
        functools.partial(attend_back_kernel, QBLOCK),
        grid=(cols // HD,),
        in_specs=[one, one, one, one, one, sums, column, row],
        out_specs=three,
        out_shape=jax.ShapeDtypeStruct((3, slots, cols), BF),
        scratch_shapes=[pltpu.VMEM((slots, HD), F32), pltpu.VMEM((slots, HD), F32)],
        cost_estimate=pl.CostEstimate(
            flops=20 * slots * slots * cols,
            bytes_accessed=16 * slots * cols,
            transcendentals=cols // HD * slots * slots,
        ),
        compiler_params=pltpu.CompilerParams(vmem_limit_bytes=40 << 20),
    )(*proj, mixed, grad, log_sum, query_place, key_place)


def norm_parts(rows):
    mean = jnp.mean(rows, axis=-1, keepdims=True)
    centred = rows - mean
    var = jnp.mean(centred * centred, axis=-1, keepdims=True)
    inv = lax.rsqrt(var + EPS)
    return centred * inv, inv


def norm_back(grad, gain, unit, inv):
    e = grad * gain
    mean_e = jnp.mean(e, axis=-1, keepdims=True)
    mean_ex = jnp.mean(e * unit, axis=-1, keepdims=True)
    return inv * (e - mean_e - unit * mean_ex)


def bit_list(n):
    return [1 << b for b in range(n.bit_length() - 1)]


def bit_reverse(i, n):
    out = 0
    for b in bit_list(n):
        out = out * 2 + (1 if i & b else 0)
    return out


class Plan:
    def __init__(self, n_dp, n_mod, micro):
        self.group = n_mod
        self.slabs = n_dp // n_mod
        self.n_mod = n_mod
        self.micro = micro
        self.span = n_mod // micro
        self.owner = [bit_reverse(z, n_mod) for z in range(n_mod)]

    def dev(self, y, q, z):
        return (y * self.group + q) * self.n_mod + z

    def all(self, f):
        return [
            (self.dev(y, q, z), self.dev(*f(y, q, z)))
            for y in range(self.slabs)
            for q in range(self.group)
            for z in range(self.n_mod)
        ]

    def swap_q(self, x, bit):
        return lax.ppermute(x, AXES, self.all(lambda y, q, z: (y, q ^ bit, z)))

    def swap_y(self, x, bit):
        return lax.ppermute(x, AXES, self.all(lambda y, q, z: (y ^ bit, q, z)))

    def swap_z(self, x, bit):
        return lax.ppermute(x, AXES, self.all(lambda y, q, z: (y, q, z ^ bit)))

    def everywhere(self, x):
        for bit in bit_list(self.group):
            x = x + self.swap_q(x, bit)
        for bit in bit_list(self.slabs):
            x = x + self.swap_y(x, bit)
        for bit in bit_list(self.n_mod):
            x = x + self.swap_z(x, bit)
        return x

    def over_dp(self, x, d):
        x = x[None]
        for bit in bit_list(self.group):
            x = jnp.concatenate([x, self.swap_q(x, bit)], axis=0)
        for bit in bit_list(self.slabs):
            x = jnp.concatenate([x, self.swap_y(x, bit)], axis=0)
        return x[d ^ jnp.arange(x.shape[0])]

    def move(self, k):
        def to(y, q, z):
            m = (k - q // self.span) % self.micro
            return y, self.owner[z], m * self.span + q % self.span

        return self.all(to)

    def send(self, x, k):
        return lax.ppermute(x, AXES, self.move(k))

    def send_back(self, x, k):
        return lax.ppermute(x, AXES, [(b, a) for a, b in self.move(k)])

    def gather(self, x):
        blocks = {0: x}
        for bit in reversed(bit_list(self.group)):
            for r in list(blocks):
                blocks[r | bit] = self.swap_q(blocks[r], bit)
        return jnp.concatenate([blocks[r] for r in range(self.group)], axis=0)

    def scatter(self, parts):
        rows = parts.shape[0] // self.group
        held = {r: parts[r * rows : (r + 1) * rows] for r in range(self.group)}
        for bit in bit_list(self.group):
            merged = {}
            for r in held:
                if not r & bit:
                    merged[r] = held[r].astype(F32) + self.swap_q(
                        held[r | bit].astype(BF), bit
                    ).astype(F32)
            held = merged
        return held[0]

    def exchange(self, x, q):
        for bit in bit_list(self.group):
            hi, lo = self.group // (2 * bit), bit
            view = x.reshape((hi, 2, lo) + x.shape[1:])
            mine = (q // bit) % 2
            keep = lax.dynamic_index_in_dim(view, mine, 1, keepdims=False)
            give = lax.dynamic_index_in_dim(view, 1 - mine, 1, keepdims=False)
            got = self.swap_q(give, bit)
            low = jnp.where(mine == 0, keep, got)
            high = jnp.where(mine == 0, got, keep)
            x = jnp.stack([low, high], axis=1).reshape(x.shape)
        return x


def shards(plan, n_dp, n_mod, args):
    (
        tokens,
        w_qkv,
        w_out,
        w_up,
        w_down,
        gains,
        biases,
        cotangent,
        lengths,
        positions,
        flags,
        item_weights,
    ) = args
    micro, _, rows_here, width = tokens.shape
    slots = positions.shape[2]
    group, slabs, span = plan.group, plan.slabs, plan.span
    block = width // n_dp
    half = width // slabs
    d = lax.axis_index("dp")
    z = lax.axis_index("mod")
    y = d // group
    q = d % group
    head_cols = w_qkv.shape[2]
    head_sub = head_cols // group
    ffn_cols = w_up.shape[1]
    ffn_sub = ffn_cols // group

    def turn(x):
        parts = x.reshape(x.shape[:-1] + (slabs, half))
        return jnp.concatenate(
            [
                lax.dynamic_index_in_dim(parts, y ^ r, x.ndim - 1, keepdims=False)
                for r in range(slabs)
            ],
            axis=-1,
        )

    small = jnp.concatenate(
        [
            positions.astype(F32).reshape(-1),
            gains.astype(F32).reshape(-1),
            biases.astype(F32).reshape(-1),
            lengths.astype(F32).reshape(-1),
            flags.astype(F32).reshape(-1),
            item_weights.astype(F32).reshape(-1),
        ]
    )
    every = plan.over_dp(small, d)
    cut = micro * slots
    place_all = every[:, :cut].reshape(n_dp, micro, slots)
    gain_all = every[:, cut : cut + 2 * block].reshape(n_dp, 2, block)
    bias_all = every[:, cut + 2 * block : cut + 4 * block].reshape(n_dp, 2, block)
    facts = every[:, cut + 4 * block :].reshape(n_dp, 3, micro)
    gain_vals = turn(jnp.swapaxes(gain_all, 0, 1).reshape(2, width))
    bias_vals = turn(jnp.swapaxes(bias_all, 0, 1).reshape(2, width))
    my_micro = z // span
    order = jnp.array([plan.owner.index(i) for i in range(group)], jnp.int32)
    block_of = order[q ^ jnp.arange(group)]

    def after(x, *first):
        return lax.optimization_barrier((x,) + first)[0]

    def block_for(x, k):
        m = (k - q // span) % micro
        return turn(lax.dynamic_index_in_dim(x, m, 0, keepdims=False)[0])

    def over_mod(x, axis):
        return lax.all_gather(x, "mod", axis=axis, tiled=True)

    streams = range(micro)
    got_qkv = plan.exchange(jnp.moveaxis(w_qkv.reshape(3, block, group, head_sub), 2, 0), q)
    mine = [got_qkv[:, t].reshape(half, head_sub) for t in range(3)]
    arrived = [plan.send(block_for(after(tokens, got_qkv), k), k) for k in streams]
    near = [over_mod(mine[t], 1) for t in range(3)]
    far = [plan.swap_y(near[t], 1) for t in range(3)]

    w_out, w_up, w_down = lax.optimization_barrier((got_qkv, w_out, w_up, w_down))[1:]
    got = plan.exchange(w_out.reshape(group, head_sub, block), q)
    near_out = over_mod(jnp.swapaxes(got, 0, 1).reshape(head_sub, half), 0)
    full_out = jnp.concatenate([near_out, plan.swap_y(after(near_out, far[2]), 1)], axis=1)
    parts = jnp.swapaxes(w_up.reshape(block, group, ffn_sub), 0, 1)
    near_up = over_mod(plan.exchange(parts, q).reshape(half, ffn_sub), 1)
    far_up = plan.swap_y(near_up, 1)
    full_up = jnp.concatenate([near_up, far_up], axis=0)
    got = plan.exchange(w_down.reshape(group, ffn_sub, block), q)
    near_down = over_mod(jnp.swapaxes(got, 0, 1).reshape(ffn_sub, half), 0)
    far_down = plan.swap_y(after(near_down, far_up), 1)
    full_down = jnp.concatenate([near_down, far_down], axis=1)

    def facts_of(k):
        pair = (k - my_micro) % micro
        source = y * group + pair * span + z % span
        item = lax.dynamic_index_in_dim(place_all, source, 0, keepdims=False)
        places = lax.dynamic_index_in_dim(item, my_micro, 0, keepdims=False)
        places = places.reshape(group, rows_here)[block_of].reshape(-1)
        fact = lax.dynamic_index_in_dim(facts, source, 0, keepdims=False)
        fact = lax.dynamic_index_in_dim(fact, my_micro, 1, keepdims=False)
        scale = jnp.where(fact[1] == 1.0, fact[2] / 4.0, 1.0)
        factor = scale * (places[:rows_here] < fact[0]).astype(F32)
        key_place = jnp.where(places < fact[0], places, NOT_A_KEY)[None, :]
        return places[:, None], key_place, factor

    query_place, key_place, factor = zip(*[facts_of(k) for k in streams])

    def dot(spec, a, b):
        return jnp.einsum(spec, a, b, preferred_element_type=F32)

    rows, unit_one, inv_one, normed = [], [], [], []
    for k in streams:
        rows.append(arrived[k].astype(F32))
        unit, inv = norm_parts(rows[k])
        unit_one.append(unit)
        inv_one.append(inv)
        normed.append(plan.gather((unit * gain_vals[0] + bias_vals[0]).astype(BF)))

    grad_out = []
    for k in streams:
        moved = plan.send(block_for(after(cotangent, arrived[k]), k), k)
        grad_out.append(moved.astype(F32) * factor[k][:, None])

    proj, mixed, log_sum, partial = [], [], [], []
    for k in streams:
        proj.append(
            [
                (
                    dot("sd,dc->sc", normed[k][:, :half], near[t])
                    + dot("sd,dc->sc", normed[k][:, half:], far[t])
                ).astype(BF)
                for t in range(3)
            ]
        )
        m, s = attend(proj[k], query_place[k], key_place[k])
        mixed.append(m)
        log_sum.append(s)
        partial.append(dot("sc,cd->sd", m, full_out).astype(BF))

    grad_out_all = [plan.gather(grad_out[k].astype(BF)) for k in streams]

    hidden, unit_two, inv_two, normed_two = [], [], [], []
    for k in streams:
        hidden.append(rows[k] + plan.scatter(partial[k]))
        unit, inv = norm_parts(hidden[k])
        unit_two.append(unit)
        inv_two.append(inv)
        normed_two.append(plan.gather((unit * gain_vals[1] + bias_vals[1]).astype(BF)))

    active, slope = [], []
    for k in streams:
        act, slp = gelu_and_slope(dot("sd,df->sf", normed_two[k], full_up))
        active.append(act.astype(BF))
        slope.append(slp.astype(BF))

    def low(x):
        return x[:, :half]

    def high(x):
        return x[:, half:]

    def same(x):
        return x

    def total(spec, left, right, cut_left, cut_right):
        out = 0.0
        for a, b in zip(left, right):
            out = out + dot(spec, cut_left(a), cut_right(b))
        return out

    def give(spec, left, right, side):
        cuts = (high, same) if side == 0 else (same, high)
        return total(spec, left, right, *cuts).astype(BF)

    def keep(spec, left, right, side, other):
        cuts = (low, same) if side == 0 else (same, low)
        return (total(spec, left, right, *cuts) + other.astype(F32)).astype(BF)

    def settle(part, axis):
        return lax.psum_scatter(part, "mod", scatter_dimension=axis, tiled=True)

    give_down = give("sf,sd->fd", active, grad_out_all, 1)
    came_down = plan.swap_y(after(give_down, far_down), 1)

    grad_upper, partial = [], []
    for k in streams:
        grad_active = dot("sd,fd->sf", grad_out_all[k], full_down)
        grad_upper.append((grad_active * slope[k].astype(F32)).astype(BF))
        partial.append(dot("sf,df->sd", grad_upper[k], full_up).astype(BF))

    give_up = give("sd,sf->df", normed_two, after(grad_upper, partial), 0)
    came_up = plan.swap_y(after(give_up, came_down), 1)

    grad_hidden, grad_two, grad_hidden_all = [], [], []
    for k in streams:
        grad_two.append(plan.scatter(partial[k]))
        grad_hidden.append(
            grad_out[k] + norm_back(grad_two[k], gain_vals[1], unit_two[k], inv_two[k])
        )
        grad_hidden_all.append(plan.gather(grad_hidden[k].astype(BF)))

    ffn = []
    for k in streams:
        ffn.append(dot("sf,fd->sd", after(active[k], partial), full_down).astype(BF))
    output = []
    for k in streams:
        done = plan.scatter(after(ffn[k], grad_hidden_all[micro - 1]))
        output.append(plan.send_back(turn((hidden[k] + done).astype(BF)), k))

    grad_down = keep("sf,sd->fd", active, grad_out_all, 1, after(came_down, ffn[micro - 1]))
    grad_down = settle(grad_down, 0)

    grad_proj, partial = [], []
    full_qkv = jnp.stack([jnp.concatenate([near[t], far[t]], axis=0) for t in range(3)])
    for k in streams:
        grad_mixed = dot("sd,cd->sc", grad_hidden_all[k], full_out).astype(BF)
        grad_proj.append(
            attend_back(proj[k], mixed[k], grad_mixed, log_sum[k], query_place[k], key_place[k])
        )
        partial.append(dot("tsc,tdc->sd", grad_proj[k], full_qkv).astype(BF))

    grad_up = keep("sd,sf->df", normed_two, grad_upper, 0, after(came_up, partial[0]))
    grad_up = settle(grad_up, 1)

    came_qkv = []
    for t in range(3):
        gave = give("sd,sc->dc", normed, [after(g[t], partial) for g in grad_proj], 0)
        came_qkv.append(plan.swap_y(after(gave, came_up), 1))
    gave = give("sc,sd->cd", mixed, after(grad_hidden_all, came_up), 1)
    came_out = plan.swap_y(gave, 1)

    grad_one, input_grad = [], []
    for k in streams:
        grad_one.append(plan.scatter(partial[k]))
        g = grad_hidden[k] + norm_back(grad_one[k], gain_vals[0], unit_one[k], inv_one[k])
        input_grad.append(plan.send_back(turn(g.astype(BF)), k))

    grad_qkv = []
    for t in range(3):
        part = keep("sd,sc->dc", normed, [g[t] for g in grad_proj], 0, came_qkv[t])
        grad_qkv.append(settle(part, 1))
    grad_out_w = settle(keep("sc,sd->cd", mixed, grad_hidden_all, 1, came_out), 0)

    part = plan.exchange(jnp.swapaxes(grad_down.reshape(ffn_sub, group, block), 0, 1), q)
    grad_down = part.reshape(ffn_cols, block).astype(F32)
    part = plan.exchange(grad_up.reshape(group, block, ffn_sub), q)
    grad_up = jnp.swapaxes(part, 0, 1).reshape(block, ffn_cols).astype(F32)
    part = plan.exchange(jnp.swapaxes(grad_out_w.reshape(head_sub, group, block), 0, 1), q)
    grad_out_w = part.reshape(head_cols, block).astype(F32)
    part = jnp.stack([p.reshape(group, block, head_sub) for p in grad_qkv], axis=1)
    part = plan.exchange(part, q)
    grad_qkv = jnp.moveaxis(part, 0, 2).reshape(3, block, head_cols).astype(F32)

    def sums_of(grads, units):
        scale_sum = sum(jnp.sum(g * u, axis=0) for g, u in zip(grads, units))
        shift_sum = sum(jnp.sum(g, axis=0) for g in grads)
        both = plan.everywhere(turn(jnp.stack([scale_sum, shift_sum])))
        return lax.dynamic_slice_in_dim(both, d * block, block, 1)

    first, second = sums_of(grad_one, unit_one), sums_of(grad_two, unit_two)
    grad_gains = jnp.stack([first[0], second[0]])
    grad_biases = jnp.stack([first[1], second[1]])

    def in_order(parts):
        shift = q // span
        out = []
        for m in range(micro):
            pick = parts[m]
            for j in range(1, micro):
                pick = jnp.where(shift == j, parts[(m + j) % micro], pick)
            out.append(pick)
        return jnp.stack(out)[:, None]

    return (
        in_order(output),
        in_order(input_grad).astype(F32),
        grad_qkv,
        grad_out_w,
        grad_up,
        grad_down,
        grad_gains,
        grad_biases,
    )


def solution(mesh):
    n_dp, n_mod = mesh.shape["dp"], mesh.shape["mod"]

    def body(*args):
        plan = Plan(n_dp, n_mod, args[0].shape[0])
        return shards(plan, n_dp, n_mod, args)

    in_specs = (
        P(None, "dp", "mod", None),
        P(None, "dp", "mod"),
        P("mod", "dp"),
        P("dp", "mod"),
        P("mod", "dp"),
        P(None, "dp"),
        P(None, "dp"),
        P(None, "dp", "mod", None),
        P(None, "dp"),
        P(None, "dp", None),
        P(None, "dp"),
        P(None, "dp"),
    )
    out_specs = (
        P(None, "dp", "mod", None),
        P(None, "dp", "mod", None),
        P(None, "dp", "mod"),
        P("mod", "dp"),
        P("dp", "mod"),
        P("mod", "dp"),
        P(None, "dp"),
        P(None, "dp"),
    )
    return jax.shard_map(body, mesh=mesh, in_specs=in_specs, out_specs=out_specs, check_vma=False)
```
